32 devices in a mesh: exp: 4 (over z), hid: 8 (over y, x, core).
Axes of the slice: x: 2, y: 2, z: 4, core: 2. Of those that a mesh axis runs over, the one named last changes fastest.
Arguments:
- tokens: bfloat16 [4, 1024, 1152], P('exp', 'hid'), may hold values from -6 to 6
- route: int32 [4, 1024, 1], P('exp', 'hid'), may hold values from 0 to 3; in each aligned block of 128 rows (0 to 127, 128 to 255, ..., all dimensions but the last counted through in order) at most 40 rows name the same one
- seq_ids: int32 [4, 1024], P('exp', 'hid'), may hold values from 0 to 1, as said below
- cotangent: bfloat16 [4, 1024, 1152], P('exp', 'hid'), may hold values from -6 to 6
- gain_one: bfloat16 [1152], replicated, may hold values from 0.5 to 1.5
- gain_two: bfloat16 [1152], replicated, may hold values from 0.5 to 1.5
- in_weight: bfloat16 [1152, 4608], P(None, ('exp', 'hid')), may hold values from -0.1875 to 0.1875
- conv_weight: bfloat16 [4, 2304], P(None, ('exp', 'hid')), may hold values from -3 to 3
- conv_bias: bfloat16 [2304], P(('exp', 'hid')), may hold values from -0.5 to 0.5
- x_weight: bfloat16 [2304, 104], P(('exp', 'hid')), may hold values from -0.125 to 0.125
- dt_weight: bfloat16 [72, 2304], P(None, ('exp', 'hid')), may hold values from -0.75 to 0.75
- dt_bias: bfloat16 [2304], P(('exp', 'hid')), may hold values from -6 to -2
- a_log: bfloat16 [2304, 16], P(('exp', 'hid')), may hold values from -6 to 2.75
- skip: bfloat16 [2304], P(('exp', 'hid')), may hold values from 0.5 to 1.5
- out_weight: bfloat16 [2304, 1152], P(('exp', 'hid')), may hold values from -0.125 to 0.125
- expert_in: bfloat16 [4, 1152, 3072], P('exp', None, 'hid'), may hold values from -0.1875 to 0.1875
- expert_out: bfloat16 [4, 3072, 1152], P('exp', 'hid'), may hold values from -0.109375 to 0.109375
Outputs:
- output: bfloat16 [4, 1024, 1152], P('exp', 'hid')
- grad_tokens: float32 [4, 1024, 1152], P('exp', 'hid')
- grad_gain_one: float32 [1152], replicated
- grad_gain_two: float32 [1152], replicated
- grad_in_weight: float32 [1152, 4608], P(None, ('exp', 'hid'))
- grad_conv_weight: float32 [4, 2304], P(None, ('exp', 'hid'))
- grad_conv_bias: float32 [2304], P(('exp', 'hid'))
- grad_x_weight: float32 [2304, 104], P(('exp', 'hid'))
- grad_dt_weight: float32 [72, 2304], P(None, ('exp', 'hid'))
- grad_dt_bias: float32 [2304], P(('exp', 'hid'))
- grad_a_log: float32 [2304, 16], P(('exp', 'hid'))
- grad_skip: float32 [2304], P(('exp', 'hid'))
- grad_out_weight: float32 [2304, 1152], P(('exp', 'hid'))
- grad_expert_in: float32 [4, 1152, 3072], P('exp', None, 'hid')
- grad_expert_out: float32 [4, 3072, 1152], P('exp', 'hid')
The draws below stay inside these ranges and needn't reach their ends.
Inputs may be any that keep to these rules, and one draw needn't show every extreme that they name: `route`: the rows of one device name no expert more than 40 times; in every draw some expert is named exactly 40 times by the rows of some device. `seq_ids`: each packed row holds one or two sequences: ids start at 0 and rise by one at most once; the first row is one whole sequence; in every other row the second sequence starts at position 256 or later.
All inputs are finite; a program needn't handle non-finite values.
Results may differ from the reference program's by a relative error of at most 0.014.
Values may be sent and summed in bfloat16 or wider, within the bound.
A program may use at most 384 MiB of HBM per device.

```python
import math
from functools import partial
import jax
import jax.numpy as jnp
import numpy as np
from jax import lax

D = 1152
DI = 2304
DS = 16
DCONV = 4
RANK = 72
FF = 3072
TOK_DEV = 128
BLOCK = 32
EXPERTS = 4
CHAINS = 4
CHAIN = 1024
CAP = 40
N_HID = 8


def draw_seq_ids(key, part):
    cut_key = jax.random.fold_in(key, 11)
    edge_key = jax.random.fold_in(key, 23)
    nudge_key = jax.random.fold_in(key, 37)
    cuts = jax.random.randint(cut_key, (CHAINS, 1), CHAIN // 4, CHAIN)
    lowest = (CHAIN // 4 + TOK_DEV - 1) // TOK_DEV
    edges = jax.random.randint(edge_key, (2,), lowest, CHAIN // TOK_DEV) * TOK_DEV
    nudge = jax.random.randint(nudge_key, (), 1, 3)
    rows = jnp.arange(CHAINS)[:, None]
    cuts = jnp.where(rows == 1, edges[0], cuts)
    cuts = jnp.where(rows == 2, edges[1] + nudge, cuts)
    cuts = jnp.where(rows == 0, CHAIN, cuts)
    positions = jnp.arange(CHAIN)[None, :]
    return (positions >= cuts).astype(jnp.int32)


def level_of(stream_key, extent, cuts, low, largest):
    loudness, own = 1.0, jax.random.fold_in(stream_key, 6)
    for axis_at, shards_of in cuts:
        heights = jnp.exp(jax.random.uniform(jax.random.fold_in(own, axis_at), (shards_of,), jnp.float32, low / len(cuts), largest / len(cuts)))
        loudness = loudness * jnp.repeat(heights, extent[axis_at] // shards_of).reshape([-1 if axis == axis_at else 1 for axis in range(len(extent))])
    return loudness


def assign_block(stream_key, own, number, rows, amount, top, bound, lean):
    order = jax.random.permutation(stream_key, amount)
    heavy_load, ordinary = shares(amount, rows * top, bound, lean, True), shares(amount, rows * top, bound, lean, False)
    places = jnp.arange(amount)

    def named(lengths, rotation):
        used = int((lengths > 0).sum())
        fixed = max(1, used // 4)
        shifted = fixed + (places - fixed + rotation * (used - fixed)) % max(1, amount - fixed)
        return jnp.zeros((amount,), jnp.int32).at[order[jnp.where(places < fixed, places, shifted)]].set(jnp.asarray(lengths, jnp.int32))

    lengths = jnp.where(number % 4 == 0, named(heavy_load, number // 4), named(ordinary, number - number // 4 - 1))
    mixed = jax.random.permutation(jax.random.fold_in(own, 3), amount)
    donor, receiver = mixed[0:amount // 2 * 2:2], mixed[1:amount // 2 * 2:2]
    slack = jnp.minimum(lengths[donor] - 1, bound - lengths[receiver]) // 2
    slack = jnp.where((donor == order[0]) | (receiver == order[0]) | (lengths[receiver] == 0), 0, jnp.maximum(slack, 0))
    shifted = jax.random.randint(jax.random.fold_in(own, 4), (amount // 2,), 0, 1 << 20) % (slack + 1)
    lengths = lengths.at[donor].add(-shifted).at[receiver].add(shifted)
    labels = jnp.searchsorted(jnp.cumsum(lengths), jnp.arange(rows * top), side="right").astype(jnp.int32)
    table = labels.reshape(top, rows).T
    table = table[jax.random.permutation(jax.random.fold_in(own, 1), rows)]
    rotation = jax.random.randint(jax.random.fold_in(own, 2), (rows, 1), 0, top)
    return jnp.take_along_axis(table, (jnp.arange(top)[None, :] + rotation) % top, axis=1)


def shares(count, total, most, lean, full):
    loads = [(1 << 20) // math.isqrt(grade ** lean) + 1 for grade in range(1, count + 1)]
    largest = most if full else min(most, max(-(-total // count), total * loads[0] // sum(loads)))
    least = 1 if total - largest >= count - 1 else 0
    given, rest = [largest] + [least] * (count - 1), total - largest - least * (count - 1)
    while rest > 0:
        free = [i for i in range(1, count) if given[i] < largest] or [i for i in range(1, count) if given[i] < most]
        mass, budget = sum([loads[i] for i in free]), rest
        for i in free:
            more = min(most - given[i], max(1, budget * loads[i] // mass), rest)
            given[i] = given[i] + more
            rest = rest - more
    return np.array(given)


def centred(own_key, shape, spread, limit, cuts=(), kind=jnp.bfloat16):
    entries = spread * jax.random.normal(own_key, shape, jnp.float32)
    if cuts:
        entries = entries * level_of(own_key, shape, cuts, -0.22, 0.18)
    return jnp.clip(entries, -limit, limit).astype(kind)


def setup_inputs(seed: int = 0) -> dict:
    arg_keys = jax.random.split(jax.random.key(seed), 18)
    tokens = centred(arg_keys[0], (CHAINS, CHAIN, D), 1.0, 6.0, ((0, 4), (1, 8)))
    route_keys = jax.random.split(jax.random.fold_in(arg_keys[1], 1), CHAINS * CHAIN // TOK_DEV)
    route_turns = jax.random.permutation(jax.random.fold_in(arg_keys[1], 3), CHAINS * CHAIN // TOK_DEV)
    route = jax.vmap(lambda own, number: assign_block(jax.random.fold_in(arg_keys[1], 2), own, number, TOK_DEV, EXPERTS, 1, CAP, 1))(route_keys, route_turns).reshape((CHAINS, CHAIN, 1))
    seq_ids = draw_seq_ids(jax.random.fold_in(arg_keys[17], 71), 0)
    cotangent = centred(arg_keys[3], (CHAINS, CHAIN, D), 1.0, 6.0, ((0, 4), (1, 8)))
    gain_one = jnp.clip(1.0 + 0.1 * jax.random.normal(arg_keys[4], (D,), jnp.float32), 0.5, 1.5).astype(jnp.bfloat16)
    gain_two = jnp.clip(1.0 + 0.1 * jax.random.normal(arg_keys[5], (D,), jnp.float32), 0.5, 1.5).astype(jnp.bfloat16)
    in_weight = centred(arg_keys[6], (D, 2 * DI), D ** -0.5, 0.1875, ((1, 32),))
    conv_weight = centred(arg_keys[7], (DCONV, DI), DCONV ** -0.5, 3.0, ((1, 32),))
    conv_bias = jnp.clip(jax.random.uniform(arg_keys[8], (DI,), jnp.float32, -0.5, 0.5) * level_of(arg_keys[8], (DI,), ((0, 32),), -0.4, 0.0), -0.5, 0.5).astype(jnp.bfloat16)
    x_weight = centred(arg_keys[9], (DI, RANK + 2 * DS), DI ** -0.5, 0.125, ((0, 32),))
    dt_weight = centred(arg_keys[10], (RANK, DI), RANK ** -0.5, 0.75, ((1, 32),))
    dt_bias = jnp.clip(-6.0 + 4.0 * jax.random.uniform(arg_keys[11], (DI,), jnp.float32) ** level_of(arg_keys[11], (DI,), ((0, 32),), -0.2, 0.2), -6.0, -2.0).astype(jnp.bfloat16)
    a_log = jnp.clip(-6.0 + 8.75 * jax.random.uniform(arg_keys[12], (DI, DS), jnp.float32) ** level_of(arg_keys[12], (DI, DS), ((0, 32),), -0.2, 0.2), -6.0, 2.75).astype(jnp.bfloat16)
    skip = jnp.clip(0.5 + 1.0 * jax.random.uniform(arg_keys[13], (DI,), jnp.float32) ** level_of(arg_keys[13], (DI,), ((0, 32),), -0.2, 0.2), 0.5, 1.5).astype(jnp.bfloat16)
    out_weight = centred(arg_keys[14], (DI, D), DI ** -0.5, 0.125, ((0, 32),))
    expert_in = centred(arg_keys[15], (EXPERTS, D, FF), D ** -0.5, 0.1875, ((0, 4), (2, 8)))
    expert_out = centred(arg_keys[16], (EXPERTS, FF, D), FF ** -0.5, 0.109375, ((0, 4), (1, 8)))
    return dict(tokens=tokens, route=route, seq_ids=seq_ids, cotangent=cotangent, gain_one=gain_one, gain_two=gain_two, in_weight=in_weight, conv_weight=conv_weight, conv_bias=conv_bias, x_weight=x_weight, dt_weight=dt_weight, dt_bias=dt_bias, a_log=a_log, skip=skip, out_weight=out_weight, expert_in=expert_in, expert_out=expert_out)


EPSILON = 1e-05
HIGHEST = lax.Precision.HIGHEST

@jax.custom_vjp
def low(v):
    return lax.optimization_barrier(v.astype(jnp.bfloat16)).astype(jnp.float32)

@jax.custom_vjp
def low_back(v):
    return v

def low_keep(v):
    return (low(v), None)

def low_pass(kept, grad):
    return (grad,)

def back_keep(v):
    return (v, None)

def back_low(kept, grad):
    return (low(grad),)
low.defvjp(low_keep, low_pass)
low_back.defvjp(back_keep, back_low)

def matmul(left_side, right_side):
    return jnp.dot(left_side, right_side, precision=HIGHEST)

def rms_scale(values, gain_vec):
    inverse = lax.rsqrt(lax.optimization_barrier(jnp.mean(values * values, axis=-1, keepdims=True)) + EPSILON)
    return values * inverse * gain_vec

def chain_combine(earlier, latter):
    return (earlier[0] * latter[0], latter[0] * earlier[1] + latter[1])

def by_blocks(values):
    return values.reshape((values.shape[0] // BLOCK, BLOCK) + values.shape[1:])

def scan_block(carried, block_in, a_matrix):
    step_size, drive_in, b_proj, c_proj, carries_on = block_in
    decays = jnp.exp(step_size[:, :, None] * a_matrix[None]) * carries_on[:, None, None]
    drives = drive_in[:, :, None] * b_proj[:, None, :]
    products, states = lax.associative_scan(chain_combine, (decays, drives), axis=0)
    states = states + products * carried[None]
    return (states[-1], lax.optimization_barrier(jnp.sum(states * c_proj[:, None, :], axis=2)))

def selective(step_size, drive_in, b_proj, c_proj, carries_on, a_matrix):
    stepper = jax.checkpoint(partial(scan_block, a_matrix=a_matrix))
    start_state = jnp.zeros((DI, DS), jnp.float32)
    pieces = tuple((by_blocks(values) for values in (step_size, drive_in, b_proj, c_proj, carries_on)))
    _, outputs = lax.scan(stepper, start_state, pieces)
    return outputs.reshape(step_size.shape)

def expert_apply(piece_rows, first_weight, second_weight):
    pre_act = low_back(matmul(piece_rows, first_weight))
    hidden_low = low(jax.nn.gelu(pre_act, approximate=False))
    return low(matmul(hidden_low, second_weight))

def mixture(normed, chosen, expert_in, expert_out):
    length = normed.shape[0]
    span = N_HID * CAP
    order = jnp.argsort(chosen, stable=True).astype(jnp.int32)
    picks = (chosen[:, None] == jnp.arange(EXPERTS, dtype=jnp.int32)[None]).astype(jnp.int32)
    counts = lax.optimization_barrier(jnp.sum(picks, axis=0)).astype(jnp.int32)
    starts = (jnp.cumsum(counts) - counts).astype(jnp.int32)
    grouped = jnp.concatenate([normed[order], jnp.zeros((span, D), jnp.float32)], axis=0)
    applier = jax.checkpoint(expert_apply)

    def one_expert(totals, expert_idx):
        first_row = starts[expert_idx].astype(jnp.int32)
        piece_rows = lax.dynamic_slice_in_dim(grouped, first_row, span, 0)
        live = (jnp.arange(span, dtype=jnp.int32) < counts[expert_idx]).astype(jnp.float32)[:, None]
        result = applier(piece_rows * live, expert_in[expert_idx], expert_out[expert_idx]) * live
        current = lax.dynamic_slice_in_dim(totals, first_row, span, 0)
        return (lax.dynamic_update_slice_in_dim(totals, current + result, first_row, 0), None)
    totals, _ = lax.scan(one_expert, jnp.zeros((length + span, D), jnp.float32), jnp.arange(EXPERTS, dtype=jnp.int32))
    inverse = jnp.zeros((length,), jnp.int32).at[order].set(jnp.arange(length, dtype=jnp.int32))
    return totals[:length][inverse]

def layer(x_rows, chosen, seq_row, gain_one, gain_two, in_weight, conv_weight, conv_bias, x_weight, dt_weight, dt_bias, a_log, skip, out_weight, expert_in, expert_out):
    length = x_rows.shape[0]
    normed_one = low(rms_scale(x_rows, gain_one))
    proj_both = low_back(matmul(normed_one, in_weight))
    conv_in = proj_both[:, :DI]
    gate_in = proj_both[:, DI:]
    rim_rows = DCONV - 1
    padded = jnp.concatenate([jnp.zeros((rim_rows, DI), jnp.float32), conv_in], axis=0)
    seq_padded = jnp.concatenate([jnp.full((rim_rows,), -1, jnp.int32), seq_row], axis=0)
    conv_out = conv_bias[None] + jnp.zeros_like(conv_in)
    matches = []
    for k in range(DCONV):
        agree = (seq_padded[k:k + length] == seq_row).astype(jnp.float32)
        matches.append(agree)
        conv_out = conv_out + conv_weight[k][None] * agree[:, None] * padded[k:k + length]
    activated = jax.nn.silu(conv_out)
    x_double = low_back(matmul(low(activated), x_weight))
    dt_low = low(x_double[:, :RANK])
    b_proj = x_double[:, RANK:RANK + DS]
    c_proj = x_double[:, RANK + DS:]
    step_size = jax.nn.softplus(low_back(matmul(dt_low, dt_weight) + dt_bias[None]))
    a_matrix = -jnp.exp(a_log)
    scanned = selective(step_size, step_size * activated, b_proj, c_proj, matches[DCONV - 2], a_matrix)
    mixed = (scanned + skip[None] * activated) * jax.nn.silu(gate_in)
    hidden_one = x_rows + low_back(matmul(low(mixed), out_weight))
    normed_two = low(low_back(rms_scale(hidden_one, gain_two)))
    return hidden_one + mixture(normed_two, chosen, expert_in, expert_out)

def reference(tokens, route, seq_ids, cotangent, gain_one, gain_two, in_weight, conv_weight, conv_bias, x_weight, dt_weight, dt_bias, a_log, skip, out_weight, expert_in, expert_out):
    weights = tuple((w.astype(jnp.float32) for w in (gain_one, gain_two, in_weight, conv_weight, conv_bias, x_weight, dt_weight, dt_bias, a_log, skip, out_weight, expert_in, expert_out)))

    def per_chain(sums, chain_in):
        x_rows, chosen, seq_row, back_rows = chain_in

        def closed(x_input, *params):
            return layer(x_input, chosen, seq_row, *params)
        result, pull = jax.vjp(closed, x_rows.astype(jnp.float32), *weights)
        grads = pull(back_rows.astype(jnp.float32))
        sums = tuple((s + g for s, g in zip(sums, grads[1:])))
        return (sums, (result.astype(jnp.bfloat16), grads[0]))
    zeros = tuple((jnp.zeros_like(w) for w in weights))
    sums, (outputs, grad_tokens) = lax.scan(per_chain, zeros, (tokens, route[:, :, 0], seq_ids, cotangent))
    return (outputs, grad_tokens, sums[0], sums[1], sums[2], sums[3], sums[4], sums[5], sums[6], sums[7], sums[8], sums[9], sums[10], sums[11], sums[12])
```

```python
import functools

import jax
import jax.numpy as jnp
from jax import lax
from jax.experimental import pallas as pl
from jax.experimental.pallas import tpu as pltpu
from jax.sharding import PartitionSpec as P

EPSILON = 1e-05
ROOT_HALF = 0.7071067811865476
INV_ROOT_TWO_PI = 0.3989422804014327
LOG2_E = 1.4426950408889634
LN_2 = 0.6931471805599453
CUT_STEP = 1e6
SUB = 16


def rms_scale(values, gain_vec):
    inverse = lax.rsqrt(jnp.mean(values * values, axis=-1, keepdims=True) + EPSILON)
    return values * inverse * gain_vec


def gelu_slope(values):
    cumulative = 0.5 * (1.0 + jax.scipy.special.erf(values * ROOT_HALF))
    return cumulative + values * INV_ROOT_TWO_PI * jnp.exp(-0.5 * values * values)


def silu_slope(values):
    sigmoid_of = jax.nn.sigmoid(values)
    return sigmoid_of + values * sigmoid_of * (1.0 - sigmoid_of)


def mat_nn(left_side, right_side):
    return jnp.dot(left_side, right_side, preferred_element_type=jnp.float32)


def mat_tn(left_side, right_side):
    return lax.dot_general(
        left_side, right_side, (((0,), (0,)), ((), ())), preferred_element_type=jnp.float32
    )


def mat_nt(left_side, right_side):
    return lax.dot_general(
        left_side, right_side, (((1,), (1,)), ((), ())), preferred_element_type=jnp.float32
    )


def group_ones(states):
    rows = lax.broadcasted_iota(jnp.int32, (SUB, SUB * states), 0)
    cols = lax.broadcasted_iota(jnp.int32, (SUB, SUB * states), 1)
    low = rows * states
    return jnp.where((cols >= low) & (cols < low + states), 1.0, 0.0).astype(jnp.bfloat16)


def scan_fwd_kernel(step_ref, drive_ref, bc_ref, a_ref, y_ref, start_ref, state, prod):
    states, _ = a_ref.shape
    block = step_ref.shape[0]

    @pl.when(pl.program_id(0) == 0)
    def _():
        state[...] = jnp.zeros_like(state)

    start_ref[0] = state[...]
    a_val = a_ref[...]

    def sub(k, s):
        base = pl.multiple_of(k * SUB, SUB)
        bc = bc_ref[k]
        for tt in range(SUB):
            row = base + tt
            decay = jnp.exp2(step_ref[pl.ds(row, 1), :] * a_val)
            s = decay * s + bc[:states, tt : tt + 1] * drive_ref[pl.ds(row, 1), :]
            at = pl.multiple_of(row * states, states)
            prod[pl.ds(at, states), :] = (s * bc[states:, tt : tt + 1]).astype(jnp.bfloat16)
        return s

    state[...] = lax.fori_loop(0, block // SUB, sub, state[...])
    ones = group_ones(states)
    for k in range(block // SUB):
        y_ref[k * SUB : (k + 1) * SUB, :] = mat_nn(
            ones, prod[k * SUB * states : (k + 1) * SUB * states, :]
        )


def scan_bwd_kernel(
    step_ref,
    drive_ref,
    grad_ref,
    bc_ref,
    a_ref,
    start_ref,
    gdrive_ref,
    gstep_ref,
    gb_ref,
    gc_ref,
    ga_ref,
    carry,
    decays,
    before,
    prod_b,
    prod_c,
    prod_d,
    prod_s,
):
    states, _ = a_ref.shape
    block = step_ref.shape[0]

    @pl.when(pl.program_id(0) == 0)
    def _():
        carry[...] = jnp.zeros_like(carry)
        ga_ref[...] = jnp.zeros_like(ga_ref)

    a_val = a_ref[...]

    def ahead(k, s):
        base = pl.multiple_of(k * SUB, SUB)
        bc = bc_ref[k]
        for tt in range(SUB):
            row = base + tt
            decay = jnp.exp2(step_ref[pl.ds(row, 1), :] * a_val)
            decays[row] = decay
            before[row] = s
            s = decay * s + bc[:states, tt : tt + 1] * drive_ref[pl.ds(row, 1), :]
            at = pl.multiple_of(row * states, states)
            prod_c[pl.ds(at, states), :] = (s * grad_ref[pl.ds(row, 1), :]).astype(jnp.bfloat16)
        return s

    lax.fori_loop(0, block // SUB, ahead, start_ref[0])

    def back(turn, held):
        q, ga = held
        k = block // SUB - 1 - turn
        base = pl.multiple_of(k * SUB, SUB)
        bc = bc_ref[k]
        for tt in reversed(range(SUB)):
            row = base + tt
            at = pl.multiple_of(row * states, states)
            adjoint = grad_ref[pl.ds(row, 1), :] * bc[states:, tt : tt + 1] + q
            prod_b[pl.ds(at, states), :] = (adjoint * drive_ref[pl.ds(row, 1), :]).astype(
                jnp.bfloat16
            )
            prod_d[pl.ds(at, states), :] = (adjoint * bc[:states, tt : tt + 1]).astype(
                jnp.bfloat16
            )
            q = decays[row] * adjoint
            pulled = q * before[row]
            ga = ga + pulled * step_ref[pl.ds(row, 1), :]
            prod_s[pl.ds(at, states), :] = (pulled * a_val).astype(jnp.bfloat16)
        return q, ga

    q, ga = lax.fori_loop(0, block // SUB, back, (carry[...], ga_ref[...]))
    carry[...] = q
    ga_ref[...] = ga
    ones = group_ones(states)
    lane_ones = jnp.ones((8, a_val.shape[1]), jnp.bfloat16)
    for k in range(block // SUB):
        rows = slice(k * SUB * states, (k + 1) * SUB * states)
        gdrive_ref[k * SUB : (k + 1) * SUB, :] = mat_nn(ones, prod_d[rows, :])
        gstep_ref[k * SUB : (k + 1) * SUB, :] = mat_nn(ones, prod_s[rows, :])
        gb_ref[0, :, rows] = mat_nt(lane_ones, prod_b[rows, :])
        gc_ref[0, :, rows] = mat_nt(lane_ones, prod_c[rows, :])


def scan_forward(step_cut, drive, bc, a_two, block):
    length, width = step_cut.shape
    states = a_two.shape[0]
    turns = length // block
    rows = pl.BlockSpec((block, width), lambda i: (i, 0))
    cost = pl.CostEstimate(
        flops=8 * length * width * states,
        transcendentals=length * width * states,
        bytes_accessed=12 * length * width,
    )
    return pl.pallas_call(
        scan_fwd_kernel,
        grid=(turns,),
        in_specs=[
            rows,
            rows,
            pl.BlockSpec((block // SUB, 2 * states, SUB), lambda i: (i, 0, 0)),
            pl.BlockSpec((states, width), lambda i: (0, 0)),
        ],
        out_specs=[rows, pl.BlockSpec((1, states, width), lambda i: (i, 0, 0))],
        out_shape=[
            jax.ShapeDtypeStruct((length, width), jnp.float32),
            jax.ShapeDtypeStruct((turns, states, width), jnp.float32),
        ],
        scratch_shapes=[
            pltpu.VMEM((states, width), jnp.float32),
            pltpu.VMEM((block * states, width), jnp.bfloat16),
        ],
        cost_estimate=cost,
        name="scan_forward",
    )(step_cut, drive, bc, a_two)


def scan_backward(step_cut, drive, grad, bc, a_two, starts, block):
    length, width = step_cut.shape
    states = a_two.shape[0]
    turns = length // block
    rows = pl.BlockSpec((block, width), lambda i: (turns - 1 - i, 0))
    flat = pl.BlockSpec((1, 8, block * states), lambda i: (turns - 1 - i, 0, 0))
    whole = pl.BlockSpec((states, width), lambda i: (0, 0))
    cost = pl.CostEstimate(
        flops=24 * length * width * states,
        transcendentals=length * width * states,
        bytes_accessed=20 * length * width,
    )
    product = pltpu.VMEM((block * states, width), jnp.bfloat16)
    history = pltpu.VMEM((block, states, width), jnp.float32)
    return pl.pallas_call(
        scan_bwd_kernel,
        grid=(turns,),
        in_specs=[
            rows,
            rows,
            rows,
            pl.BlockSpec((block // SUB, 2 * states, SUB), lambda i: (turns - 1 - i, 0, 0)),
            whole,
            pl.BlockSpec((1, states, width), lambda i: (turns - 1 - i, 0, 0)),
        ],
        out_specs=[rows, rows, flat, flat, whole],
        out_shape=[
            jax.ShapeDtypeStruct((length, width), jnp.float32),
            jax.ShapeDtypeStruct((length, width), jnp.float32),
            jax.ShapeDtypeStruct((turns, 8, block * states), jnp.float32),
            jax.ShapeDtypeStruct((turns, 8, block * states), jnp.float32),
            jax.ShapeDtypeStruct((states, width), jnp.float32),
        ],
        scratch_shapes=[
            pltpu.VMEM((states, width), jnp.float32),
            history,
            history,
            product,
            product,
            product,
            product,
        ],
        cost_estimate=cost,
        name="scan_backward",
    )(step_cut, drive, grad, bc, a_two, starts)


def routing(exp_count, hid_count):
    pairs = []
    for j in range(exp_count * hid_count):
        half, bit = j // 2, j % 2
        pairs.append((j, (2 * (half // hid_count) + bit) * hid_count + half % hid_count))
    return pairs


def per_device(
    tokens,
    route,
    seq_ids,
    cotangent,
    gain_one,
    gain_two,
    in_weight,
    conv_weight,
    conv_bias,
    x_weight,
    dt_weight,
    dt_bias,
    a_log,
    skip,
    out_weight,
    expert_in,
    expert_out,
):
    both = ("exp", "hid")
    exp_count = lax.axis_size("exp")
    hid_count = lax.axis_size("hid")
    row_count = tokens.shape[1]
    model_width = tokens.shape[2]
    own = x_weight.shape[0]
    width = own * exp_count
    length = row_count * hid_count
    rank = dt_weight.shape[0]
    states = a_log.shape[1]
    taps = conv_weight.shape[0]
    pairs = routing(exp_count, hid_count)

    x_rows = tokens[0].astype(jnp.float32)
    gain_first = gain_one.astype(jnp.float32)
    gain_second = gain_two.astype(jnp.float32)
    back_low = cotangent[0]

    small = jnp.concatenate(
        [
            x_weight,
            dt_weight.T,
            a_log,
            conv_weight.T,
            conv_bias[:, None],
            dt_bias[:, None],
            skip[:, None],
        ],
        axis=1,
    )
    small_width = small.shape[1]
    pad = -small_width % 128
    packed = jnp.concatenate(
        [out_weight, small, jnp.zeros((own, pad), jnp.bfloat16)], axis=1
    )
    routed = lax.ppermute(packed, both, pairs)
    w_in = lax.all_gather(in_weight.T, "exp", axis=0, tiled=True)
    w_all = lax.all_gather(routed, "exp", axis=0, tiled=True)
    w_conv_in, w_gate = w_in[:width], w_in[width:]
    w_out = w_all[:, :model_width]
    w_small = w_all[:, model_width:]
    at = 0
    w_x = w_small[:, at : at + rank + 2 * states]
    at += rank + 2 * states
    w_dt = w_small[:, at : at + rank]
    at += rank
    alog_rows = w_small[:, at : at + states]
    at += states
    tap_rows = w_small[:, at : at + taps].astype(jnp.float32).T
    at += taps
    conv_shift = w_small[:, at].astype(jnp.float32)
    step_bias = w_small[:, at + 1].astype(jnp.float32)
    skip_gain = w_small[:, at + 2].astype(jnp.float32)
    a_neg = -jnp.exp(alog_rows.astype(jnp.float32)).T
    a_two = a_neg * LOG2_E

    normed_low = lax.all_gather(
        rms_scale(x_rows, gain_first).astype(jnp.bfloat16), "hid", axis=0, tiled=True
    )
    seq_row = lax.all_gather(seq_ids[0], "hid", axis=0, tiled=True)
    conv_in = mat_nt(normed_low, w_conv_in)
    gate_in = mat_nt(normed_low, w_gate)
    rim = taps - 1
    ext_rows = jnp.concatenate([jnp.zeros((rim, width), jnp.float32), conv_in], axis=0)
    ext_seq = jnp.concatenate([jnp.full((rim,), -1, jnp.int32), seq_row], axis=0)
    matches = [
        (ext_seq[k : k + length] == seq_row).astype(jnp.float32)[:, None] for k in range(taps)
    ]
    conv_out = conv_shift[None] + jnp.zeros_like(conv_in)
    for k in range(taps):
        conv_out = conv_out + tap_rows[k][None] * matches[k] * ext_rows[k : k + length]
    activated = jax.nn.silu(conv_out)
    act_low = activated.astype(jnp.bfloat16)
    x_double = lax.psum(mat_nn(act_low, w_x), "hid")
    dt_low = x_double[:, :rank].astype(jnp.bfloat16)
    bc = x_double[:, rank:].reshape(length // SUB, SUB, 2 * states).transpose(0, 2, 1)
    pre_step = mat_nt(dt_low, w_dt) + step_bias[None]
    step_size = jax.nn.softplus(pre_step)
    step_cut = jnp.where(matches[taps - 2] > 0.5, step_size, CUT_STEP)
    drive = step_size * activated
    scanned, starts = scan_forward(step_cut, drive, bc, a_two, row_count)
    state_out = scanned + skip_gain[None] * activated
    gate_silu = jax.nn.silu(gate_in)
    mixed_low = (state_out * gate_silu).astype(jnp.bfloat16)
    mixed_sum = lax.psum_scatter(
        mat_nn(mixed_low, w_out).astype(jnp.bfloat16), "hid", scatter_dimension=0, tiled=True
    )
    hidden_one = x_rows + mixed_sum.astype(jnp.float32)
    two_low = rms_scale(hidden_one, gain_second).astype(jnp.bfloat16)

    capacity = 5 * row_count // (4 * exp_count)
    slot_count = exp_count * capacity
    chosen = route[0, :, 0]
    picks = (chosen[:, None] == jnp.arange(exp_count, dtype=jnp.int32)[None]).astype(jnp.int32)
    ranks = jnp.cumsum(picks, axis=0) - 1
    slot_of = jnp.sum(picks * ranks, axis=1)
    place = (
        (chosen * capacity + slot_of)[:, None] == jnp.arange(slot_count, dtype=jnp.int32)[None]
    ).astype(jnp.bfloat16)

    def to_expert(rows):
        slots = mat_tn(place, rows).astype(jnp.bfloat16)
        slots = slots.reshape(exp_count, capacity, model_width)
        got = lax.all_to_all(slots, "exp", split_axis=0, concat_axis=0, tiled=True)
        got = got.reshape(slot_count, model_width)
        return lax.all_gather(got, "hid", axis=0, tiled=True)

    grads_piece = to_expert(back_low)
    rows_piece = to_expert(two_low)
    first_slice = expert_in[0]
    second_slice = expert_out[0]
    pre_act = mat_nn(rows_piece, first_slice)
    hidden_piece = jax.nn.gelu(pre_act, approximate=False).astype(jnp.bfloat16)
    grad_piece = (mat_nt(grads_piece, second_slice) * gelu_slope(pre_act)).astype(jnp.bfloat16)
    grad_first = mat_tn(rows_piece, grad_piece)[None]
    grad_second = mat_tn(hidden_piece, grads_piece)[None]
    summed = lax.psum_scatter(
        jnp.concatenate(
            [mat_nn(hidden_piece, second_slice), mat_nt(grad_piece, first_slice)], axis=1
        ).astype(jnp.bfloat16),
        "hid",
        scatter_dimension=0,
        tiled=True,
    )
    returned = lax.all_to_all(
        summed.reshape(exp_count, capacity, 2 * model_width),
        "exp",
        split_axis=0,
        concat_axis=0,
        tiled=True,
    ).reshape(slot_count, 2 * model_width)
    spread = mat_nn(place, returned)
    branch_two = spread[:, :model_width]
    grad_normed = spread[:, model_width:]
    result = (hidden_one + branch_two).astype(jnp.bfloat16)[None]
    _, norm_two_pull = jax.vjp(rms_scale, hidden_one, gain_second)
    grad_h_norm, grad_gain_second = norm_two_pull(grad_normed)
    grad_hidden = back_low.astype(jnp.float32) + grad_h_norm

    grad_mix = lax.all_gather(grad_hidden.astype(jnp.bfloat16), "hid", axis=0, tiled=True)
    grad_out_w = mat_tn(mixed_low, grad_mix)
    grad_mixed = mat_nt(grad_mix, w_out)
    grad_state_out = grad_mixed * gate_silu
    grad_gate = (grad_mixed * state_out * silu_slope(gate_in)).astype(jnp.bfloat16)
    grad_skip = jnp.sum(grad_state_out * activated, axis=0)
    grad_drive, grad_cut, gb_flat, gc_flat, grad_amat = scan_backward(
        step_cut, drive, grad_state_out, bc, a_two, starts, row_count
    )
    grad_b = gb_flat[:, 0, :].reshape(length, states)
    grad_c = gc_flat[:, 0, :].reshape(length, states)
    grad_step = grad_cut * LN_2 + grad_drive * activated
    grad_act = grad_state_out * skip_gain[None] + grad_drive * step_size
    grad_pre_step = (grad_step * jax.nn.sigmoid(pre_step)).astype(jnp.bfloat16)
    grad_dt_bias = jnp.sum(grad_pre_step.astype(jnp.float32), axis=0)
    grad_dt_w = mat_tn(grad_pre_step, dt_low)
    grad_double = lax.psum(
        jnp.concatenate([mat_nn(grad_pre_step, w_dt), grad_b, grad_c], axis=1), "hid"
    ).astype(jnp.bfloat16)
    grad_x_w = mat_tn(act_low, grad_double)
    grad_act = grad_act + mat_nt(grad_double, w_x)
    grad_conv = grad_act * silu_slope(conv_out)
    ext_grad = jnp.concatenate([grad_conv, jnp.zeros((rim, width), jnp.float32)], axis=0)
    ext_after = jnp.concatenate([seq_row, jnp.full((rim,), -1, jnp.int32)], axis=0)
    grad_conv_in = jnp.zeros_like(grad_conv)
    tap_grads = []
    for k in range(taps):
        tap_grads.append(jnp.sum(grad_conv * matches[k] * ext_rows[k : k + length], axis=0))
        agree = (ext_after[rim - k : rim - k + length] == seq_row).astype(jnp.float32)[:, None]
        grad_conv_in = (
            grad_conv_in + tap_rows[k][None] * agree * ext_grad[rim - k : rim - k + length]
        )
    grad_conv_b = jnp.sum(grad_conv, axis=0)
    grad_conv_low = grad_conv_in.astype(jnp.bfloat16)
    grad_in_conv = mat_tn(grad_conv_low, normed_low)
    grad_in_gate = mat_tn(grad_gate, normed_low)
    grad_normed_one = lax.psum_scatter(
        (mat_nn(grad_conv_low, w_conv_in) + mat_nn(grad_gate, w_gate)).astype(jnp.bfloat16),
        "hid",
        scatter_dimension=0,
        tiled=True,
    ).astype(jnp.float32)
    _, norm_one_pull = jax.vjp(rms_scale, x_rows, gain_first)
    grad_x_norm, grad_gain_first = norm_one_pull(grad_normed_one)
    grad_tokens = (grad_hidden + grad_x_norm)[None]

    grad_small = jnp.concatenate(
        [
            grad_x_w,
            grad_dt_w,
            (grad_amat * a_neg).T,
            jnp.stack(tap_grads + [grad_conv_b, grad_dt_bias, grad_skip], axis=1),
            jnp.zeros((width, pad), jnp.float32),
        ],
        axis=1,
    )
    backs = [(target, source) for source, target in pairs]
    in_sum = lax.psum_scatter(
        jnp.concatenate([grad_in_conv, grad_in_gate], axis=0).astype(jnp.bfloat16),
        "exp",
        scatter_dimension=0,
        tiled=True,
    ).astype(jnp.float32)
    rest_sum = lax.psum_scatter(
        jnp.concatenate([grad_out_w, grad_small], axis=1), "exp", scatter_dimension=0, tiled=True
    )
    rest_own = lax.ppermute(rest_sum, both, backs)
    small_own = rest_own[:, model_width:]
    at = rank + 2 * states
    at_alog = at + rank
    at_taps = at_alog + states
    at_bias = at_taps + taps
    gain_sums = lax.psum((grad_gain_first, grad_gain_second), both)
    return (
        result,
        grad_tokens,
        gain_sums[0],
        gain_sums[1],
        in_sum.T,
        small_own[:, at_taps:at_bias].T,
        small_own[:, at_bias],
        small_own[:, :at],
        small_own[:, at:at_alog].T,
        small_own[:, at_bias + 1],
        small_own[:, at_alog:at_taps],
        small_own[:, at_bias + 2],
        rest_own[:, :model_width],
        grad_first,
        grad_second,
    )


def solution(mesh):
    flat = ("exp", "hid")
    return jax.shard_map(
        per_device,
        mesh=mesh,
        in_specs=(
            P("exp", "hid", None),
            P("exp", "hid", None),
            P("exp", "hid"),
            P("exp", "hid", None),
            P(),
            P(),
            P(None, flat),
            P(None, flat),
            P(flat),
            P(flat, None),
            P(None, flat),
            P(flat),
            P(flat, None),
            P(flat),
            P(flat, None),
            P("exp", None, "hid"),
            P("exp", "hid", None),
        ),
        out_specs=(
            P("exp", "hid", None),
            P("exp", "hid", None),
            P(),
            P(),
            P(None, flat),
            P(None, flat),
            P(flat),
            P(flat, None),
            P(None, flat),
            P(flat),
            P(flat, None),
            P(flat),
            P(flat, None),
            P("exp", None, "hid"),
            P("exp", "hid", None),
        ),
        check_vma=False,
    )
```

```python
import functools

import jax
import jax.numpy as jnp
from jax import lax
from jax.experimental import pallas as pl
from jax.experimental.pallas import tpu as pltpu
from jax.sharding import PartitionSpec as P

EPSILON = 1e-05
ROOT_HALF = 0.7071067811865476
INV_ROOT_TWO_PI = 0.3989422804014327
LOG2_E = 1.4426950408889634
LN_2 = 0.6931471805599453
CUT_STEP = 1e6
SUB = 16


def rms_scale(values, gain_vec):
    inverse = lax.rsqrt(jnp.mean(values * values, axis=-1, keepdims=True) + EPSILON)
    return values * inverse * gain_vec


def gelu_slope(values):
    cumulative = 0.5 * (1.0 + jax.scipy.special.erf(values * ROOT_HALF))
    return cumulative + values * INV_ROOT_TWO_PI * jnp.exp(-0.5 * values * values)


def silu_slope(values):
    sigmoid_of = jax.nn.sigmoid(values)
    return sigmoid_of + values * sigmoid_of * (1.0 - sigmoid_of)


def mat_nn(left_side, right_side):
    return jnp.dot(left_side, right_side, preferred_element_type=jnp.float32)


def mat_tn(left_side, right_side):
    return lax.dot_general(
        left_side, right_side, (((0,), (0,)), ((), ())), preferred_element_type=jnp.float32
    )


def mat_nt(left_side, right_side):
    return lax.dot_general(
        left_side, right_side, (((1,), (1,)), ((), ())), preferred_element_type=jnp.float32
    )


def group_ones(states):
    rows = lax.broadcasted_iota(jnp.int32, (SUB, SUB * states), 0)
    cols = lax.broadcasted_iota(jnp.int32, (SUB, SUB * states), 1)
    low = rows * states
    return jnp.where((cols >= low) & (cols < low + states), 1.0, 0.0).astype(jnp.bfloat16)


def scan_fwd_kernel(step_ref, drive_ref, bc_ref, a_ref, y_ref, start_ref, state, prod):
    states, _ = a_ref.shape
    block = step_ref.shape[0]

    @pl.when(pl.program_id(0) == 0)
    def _():
        state[...] = jnp.zeros_like(state)

    start_ref[0] = state[...]
    a_val = a_ref[...]

    def sub(k, s):
        base = pl.multiple_of(k * SUB, SUB)
        bc = bc_ref[k]
        for tt in range(SUB):
            row = base + tt
            decay = jnp.exp2(step_ref[pl.ds(row, 1), :] * a_val)
            s = decay * s + bc[:states, tt : tt + 1] * drive_ref[pl.ds(row, 1), :]
            at = pl.multiple_of(row * states, states)
            prod[pl.ds(at, states), :] = (s * bc[states:, tt : tt + 1]).astype(jnp.bfloat16)
        return s

    state[...] = lax.fori_loop(0, block // SUB, sub, state[...])
    ones = group_ones(states)
    for k in range(block // SUB):
        y_ref[k * SUB : (k + 1) * SUB, :] = mat_nn(
            ones, prod[k * SUB * states : (k + 1) * SUB * states, :]
        )


def scan_bwd_kernel(
    step_ref,
    drive_ref,
    grad_ref,
    bc_ref,
    a_ref,
    start_ref,
    gdrive_ref,
    gstep_ref,
    gb_ref,
    gc_ref,
    ga_ref,
    carry,
    decays,
    before,
    prod_b,
    prod_c,
    prod_d,
    prod_s,
):
    states, _ = a_ref.shape
    block = step_ref.shape[0]

    @pl.when(pl.program_id(0) == 0)
    def _():
        carry[...] = jnp.zeros_like(carry)
        ga_ref[...] = jnp.zeros_like(ga_ref)

    a_val = a_ref[...]

    def ahead(k, s):
        base = pl.multiple_of(k * SUB, SUB)
        bc = bc_ref[k]
        for tt in range(SUB):
            row = base + tt
            decay = jnp.exp2(step_ref[pl.ds(row, 1), :] * a_val)
            decays[row] = decay
            before[row] = s
            s = decay * s + bc[:states, tt : tt + 1] * drive_ref[pl.ds(row, 1), :]
            at = pl.multiple_of(row * states, states)
            prod_c[pl.ds(at, states), :] = (s * grad_ref[pl.ds(row, 1), :]).astype(jnp.bfloat16)
        return s

    lax.fori_loop(0, block // SUB, ahead, start_ref[0])

    def back(turn, held):
        q, ga = held
        k = block // SUB - 1 - turn
        base = pl.multiple_of(k * SUB, SUB)
        bc = bc_ref[k]
        for tt in reversed(range(SUB)):
            row = base + tt
            at = pl.multiple_of(row * states, states)
            adjoint = grad_ref[pl.ds(row, 1), :] * bc[states:, tt : tt + 1] + q
            prod_b[pl.ds(at, states), :] = (adjoint * drive_ref[pl.ds(row, 1), :]).astype(
                jnp.bfloat16
            )
            prod_d[pl.ds(at, states), :] = (adjoint * bc[:states, tt : tt + 1]).astype(
                jnp.bfloat16
            )
            q = decays[row] * adjoint
            pulled = q * before[row]
            ga = ga + pulled * step_ref[pl.ds(row, 1), :]
            prod_s[pl.ds(at, states), :] = (pulled * a_val).astype(jnp.bfloat16)
        return q, ga

    q, ga = lax.fori_loop(0, block // SUB, back, (carry[...], ga_ref[...]))
    carry[...] = q
    ga_ref[...] = ga
    ones = group_ones(states)
    lane_ones = jnp.ones((8, a_val.shape[1]), jnp.bfloat16)
    for k in range(block // SUB):
        rows = slice(k * SUB * states, (k + 1) * SUB * states)
        gdrive_ref[k * SUB : (k + 1) * SUB, :] = mat_nn(ones, prod_d[rows, :])
        gstep_ref[k * SUB : (k + 1) * SUB, :] = mat_nn(ones, prod_s[rows, :])
        gb_ref[0, :, rows] = mat_nt(lane_ones, prod_b[rows, :])
        gc_ref[0, :, rows] = mat_nt(lane_ones, prod_c[rows, :])


def scan_forward(step_cut, drive, bc, a_two, block):
    length, width = step_cut.shape
    states = a_two.shape[0]
    turns = length // block
    rows = pl.BlockSpec((block, width), lambda i: (i, 0))
    cost = pl.CostEstimate(
        flops=8 * length * width * states,
        transcendentals=length * width * states,
        bytes_accessed=12 * length * width,
    )
    return pl.pallas_call(
        scan_fwd_kernel,
        grid=(turns,),
        in_specs=[
            rows,
            rows,
            pl.BlockSpec((block // SUB, 2 * states, SUB), lambda i: (i, 0, 0)),
            pl.BlockSpec((states, width), lambda i: (0, 0)),
        ],
        out_specs=[rows, pl.BlockSpec((1, states, width), lambda i: (i, 0, 0))],
        out_shape=[
            jax.ShapeDtypeStruct((length, width), jnp.float32),
            jax.ShapeDtypeStruct((turns, states, width), jnp.float32),
        ],
        scratch_shapes=[
            pltpu.VMEM((states, width), jnp.float32),
            pltpu.VMEM((block * states, width), jnp.bfloat16),
        ],
        cost_estimate=cost,
        name="scan_forward",
    )(step_cut, drive, bc, a_two)


def scan_backward(step_cut, drive, grad, bc, a_two, starts, block):
    length, width = step_cut.shape
    states = a_two.shape[0]
    turns = length // block
    rows = pl.BlockSpec((block, width), lambda i: (turns - 1 - i, 0))
    flat = pl.BlockSpec((1, 8, block * states), lambda i: (turns - 1 - i, 0, 0))
    whole = pl.BlockSpec((states, width), lambda i: (0, 0))
    cost = pl.CostEstimate(
        flops=24 * length * width * states,
        transcendentals=length * width * states,
        bytes_accessed=20 * length * width,
    )
    product = pltpu.VMEM((block * states, width), jnp.bfloat16)
    history = pltpu.VMEM((block, states, width), jnp.float32)
    return pl.pallas_call(
        scan_bwd_kernel,
        grid=(turns,),
        in_specs=[
            rows,
            rows,
            rows,
            pl.BlockSpec((block // SUB, 2 * states, SUB), lambda i: (turns - 1 - i, 0, 0)),
            whole,
            pl.BlockSpec((1, states, width), lambda i: (turns - 1 - i, 0, 0)),
        ],
        out_specs=[rows, rows, flat, flat, whole],
        out_shape=[
            jax.ShapeDtypeStruct((length, width), jnp.float32),
            jax.ShapeDtypeStruct((length, width), jnp.float32),
            jax.ShapeDtypeStruct((turns, 8, block * states), jnp.float32),
            jax.ShapeDtypeStruct((turns, 8, block * states), jnp.float32),
            jax.ShapeDtypeStruct((states, width), jnp.float32),
        ],
        scratch_shapes=[
            pltpu.VMEM((states, width), jnp.float32),
            history,
            history,
            product,
            product,
            product,
            product,
        ],
        cost_estimate=cost,
        name="scan_backward",
    )(step_cut, drive, grad, bc, a_two, starts)


MESH = pl.DeviceIdType.MESH
IN_VMEM = pl.BlockSpec(memory_space=pltpu.VMEM)


class Place:
    def __init__(self):
        self.planes, self.peers = lax.axis_size("exp"), lax.axis_size("hid")
        self.e, self.h = lax.axis_index("exp"), lax.axis_index("hid")
        self.chips = self.peers // 2
        self.chip, self.core = self.h // 2, self.h % 2

    def hid_at(self, k):
        return (self.h + k) % self.peers

    def hid_back(self, k):
        return (self.h + self.peers - k) % self.peers

    def chip_at(self, q):
        return (self.chip + q) % self.chips

    def chip_back(self, q):
        return (self.chip + self.chips - q) % self.chips

    def plane_at(self, k):
        return (self.e + k) % self.planes

    def plane_back(self, k):
        return (self.e + self.planes - k) % self.planes

    def same_core(self, chip):
        return 2 * chip + self.core

    @property
    def sibling(self):
        return 2 * self.chip + 1 - self.core


def remote(src, dst, send, recv, plane, hid):
    return pltpu.make_async_remote_copy(
        src_ref=src,
        dst_ref=dst,
        send_sem=send,
        recv_sem=recv,
        device_id=(plane, hid),
        device_id_type=MESH,
    )


def signal(sem, plane, hid):
    pl.semaphore_signal(sem, inc=1, device_id=(plane, hid), device_id_type=MESH)


def greet(me, hid=True, exp=True):
    barrier = pltpu.get_barrier_semaphore()
    count = 0
    if hid:
        for k in range(1, me.peers):
            signal(barrier, me.e, me.hid_at(k))
        count += me.peers - 1
    if exp:
        for k in range(1, me.planes):
            signal(barrier, me.plane_at(k), me.h)
        count += me.planes - 1
    pl.semaphore_wait(barrier, count)


def comm_call(body, name, collective_id, outs, scratch, operands, sent):
    return pl.pallas_call(
        body,
        out_shape=outs,
        in_specs=[IN_VMEM] * len(operands),
        out_specs=[IN_VMEM] * len(outs),
        scratch_shapes=scratch,
        compiler_params=pltpu.CompilerParams(
            collective_id=collective_id, has_side_effects=True, vmem_limit_bytes=60 * 2**20
        ),
        cost_estimate=pl.CostEstimate(flops=0, transcendentals=0, bytes_accessed=8 * sent),
        name=name,
    )(*operands)


def dma(*shape):
    return pltpu.SemaphoreType.DMA(shape)


def size_of(array):
    return array.size * array.dtype.itemsize


def gather_start(me, x_ref, out_ref, send, recv):
    copies = []
    for q in range(1, me.chips):
        copy = remote(
            x_ref, out_ref.at[me.h], send.at[q], recv.at[q], me.e, me.same_core(me.chip_at(q))
        )
        copy.start()
        copies.append(copy)
    copy = remote(x_ref, out_ref.at[me.h], send.at[0], recv.at[0], me.e, me.sibling)
    copy.start()
    return copies + [copy]


def gather_pass_on(me, x_ref, out_ref, send, recv, pass_send, pass_recv):
    copies = []
    for q in range(1, me.chips):
        block = out_ref.at[me.same_core(me.chip_back(q))]
        remote(x_ref, block, send.at[q], recv.at[q], me.e, me.h).wait_recv()
        copy = remote(block, block, pass_send.at[q], pass_recv.at[q], me.e, me.sibling)
        copy.start()
        copies.append(copy)
    return copies


def gather_finish(me, x_ref, out_ref, send, recv, pass_send, pass_recv, copies):
    remote(x_ref, out_ref.at[me.sibling], send.at[0], recv.at[0], me.e, me.h).wait_recv()
    for q in range(1, me.chips):
        block = out_ref.at[2 * me.chip_back(q) + 1 - me.core]
        remote(block, block, pass_send.at[q], pass_recv.at[q], me.e, me.h).wait_recv()
    for copy in copies:
        copy.wait_send()


def gather_kernel(x_ref, out_ref, own_sem, send, recv, pass_send, pass_recv):
    me = Place()
    own = pltpu.make_async_copy(x_ref, out_ref.at[me.h], own_sem)
    own.start()
    greet(me, exp=False)
    copies = gather_start(me, x_ref, out_ref, send, recv)
    copies += gather_pass_on(me, x_ref, out_ref, send, recv, pass_send, pass_recv)
    gather_finish(me, x_ref, out_ref, send, recv, pass_send, pass_recv, copies)
    own.wait()


def gather_hid(x, name, collective_id):
    peers = lax.axis_size("hid")
    chips = peers // 2
    return comm_call(
        gather_kernel,
        name,
        collective_id,
        [jax.ShapeDtypeStruct((peers,) + x.shape, x.dtype)],
        [pltpu.SemaphoreType.DMA] + [dma(chips)] * 4,
        [x],
        size_of(x) * peers,
    )[0]


def start_kernel(
    normed_ref,
    seq_ref,
    conv_ref,
    small_ref,
    cot_ref,
    normed_out,
    seq_out,
    conv_out,
    small_out,
    cot_out,
    own_sem,
    send,
    recv,
    pass_send,
    pass_recv,
    seq_send,
    seq_recv,
    right_send,
    left_send,
    line_recv,
    small_send,
    small_recv,
    cot_send,
    cot_recv,
):
    me = Place()
    planes, peers = me.planes, me.peers
    sources, chunks = conv_out.shape[0], conv_out.shape[1]
    flat = me.e * peers + me.h
    half = flat // 2
    user = half % peers
    my_slot = 2 * (half // peers) + flat % 2
    self_user = user == me.h
    holds = me.e < sources

    own_normed = pltpu.make_async_copy(normed_ref, normed_out.at[me.h], own_sem.at[0])
    own_seq = pltpu.make_async_copy(seq_ref, seq_out.at[me.h], own_sem.at[1])
    own_cot = pltpu.make_async_copy(cot_ref.at[me.e], cot_out.at[me.e], own_sem.at[2])
    own_normed.start()
    own_seq.start()
    own_cot.start()

    barrier = pltpu.get_barrier_semaphore()
    for k in range(1, peers):
        signal(barrier, me.e, me.hid_at(k))
    for k in range(1, planes):
        signal(barrier, me.plane_at(k), me.h)

    def owner(s):
        j = 2 * ((s // 2) * peers + me.h) + s % 2
        return j // peers, j % peers, j != flat

    for s in range(planes):
        plane, hid, other = owner(s)

        @pl.when(other)
        def _():
            signal(barrier, plane, hid)

    pl.semaphore_wait(barrier, peers - 1 + planes - 1 + planes - self_user.astype(jnp.int32))

    copies = gather_start(me, normed_ref, normed_out, send, recv)

    def line(direction, block, chunk):
        sems = right_send if direction > 0 else left_send
        return remote(
            conv_out.at[block, chunk],
            conv_out.at[block, chunk],
            sems.at[block, chunk],
            line_recv.at[block, chunk],
            me.e + direction,
            me.h,
        )

    def line_first(direction, chunk):
        sems = right_send if direction > 0 else left_send
        return remote(
            conv_ref.at[chunk],
            conv_out.at[me.e, chunk],
            sems.at[me.e, chunk],
            line_recv.at[me.e, chunk],
            me.e + direction,
            me.h,
        )

    for chunk in range(chunks):

        @pl.when(holds & (me.e + 1 < planes))
        def _():
            line_first(1, chunk).start()

        @pl.when(holds & (me.e > 0))
        def _():
            line_first(-1, chunk).start()

    own_conv = pltpu.make_async_copy(conv_ref, conv_out.at[me.e % sources], own_sem.at[3])

    @pl.when(holds)
    def _():
        own_conv.start()

    for k in range(1, peers):
        copy = remote(
            seq_ref, seq_out.at[me.h], seq_send.at[k], seq_recv.at[k], me.e, me.hid_at(k)
        )
        copy.start()
        copies.append(copy)

    def small_copy(k):
        return remote(
            small_ref,
            small_out.at[my_slot],
            small_send.at[k],
            small_recv.at[my_slot],
            me.plane_at(k),
            user,
        )

    own_small = pltpu.make_async_copy(small_ref, small_out.at[my_slot], own_sem.at[4])
    for k in range(1, planes):
        small_copy(k).start()

    @pl.when(self_user)
    def _():
        own_small.start()

    @pl.when(user != me.h)
    def _():
        small_copy(0).start()

    for k in range(1, planes):
        copy = remote(
            cot_ref.at[me.plane_at(k)],
            cot_out.at[me.e],
            cot_send.at[k],
            cot_recv.at[k],
            me.plane_at(k),
            me.h,
        )
        copy.start()
        copies.append(copy)

    for far in range(1, planes):
        from_left, from_right = me.e - far, me.e + far
        for chunk in range(chunks):

            @pl.when((from_left >= 0) & (from_left < sources))
            def _():
                line(0, from_left, chunk).wait_recv()

                @pl.when(me.e + 1 < planes)
                def _():
                    line(1, from_left, chunk).start()

            @pl.when(from_right < sources)
            def _():
                line(0, from_right, chunk).wait_recv()

                @pl.when(me.e > 0)
                def _():
                    line(-1, from_right, chunk).start()

        if far == 1:
            copies += gather_pass_on(
                me, normed_ref, normed_out, send, recv, pass_send, pass_recv
            )

    gather_finish(me, normed_ref, normed_out, send, recv, pass_send, pass_recv, copies)
    for k in range(1, peers):
        remote(
            seq_ref,
            seq_out.at[me.hid_back(k)],
            seq_send.at[k],
            seq_recv.at[k],
            me.e,
            me.h,
        ).wait_recv()
    for s in range(planes):
        _, _, other = owner(s)

        @pl.when(other)
        def _():
            remote(
                small_ref, small_out.at[s], small_send.at[0], small_recv.at[s], me.e, me.h
            ).wait_recv()

    for k in range(1, planes):
        remote(
            cot_ref.at[me.e],
            cot_out.at[me.plane_back(k)],
            cot_send.at[k],
            cot_recv.at[k],
            me.e,
            me.h,
        ).wait_recv()
    for k in range(1, planes):
        small_copy(k).wait_send()

    @pl.when(user != me.h)
    def _():
        small_copy(0).wait_send()

    @pl.when(self_user)
    def _():
        own_small.wait()

    for chunk in range(chunks):

        @pl.when(holds & (me.e + 1 < planes))
        def _():
            line_first(1, chunk).wait_send()

        @pl.when(holds & (me.e > 0))
        def _():
            line_first(-1, chunk).wait_send()

        for far in range(1, planes):
            from_left, from_right = me.e - far, me.e + far

            @pl.when((from_left >= 0) & (from_left < sources) & (me.e + 1 < planes))
            def _():
                line(1, from_left, chunk).wait_send()

            @pl.when((from_right < sources) & (me.e > 0))
            def _():
                line(-1, from_right, chunk).wait_send()

    @pl.when(holds)
    def _():
        own_conv.wait()

    own_normed.wait()
    own_seq.wait()
    own_cot.wait()


def start_gather(normed, seq, conv, small, cot):
    planes, peers = lax.axis_size("exp"), lax.axis_size("hid")
    chips, sources, chunks = peers // 2, planes // 2, conv.shape[0]
    shaped = jax.ShapeDtypeStruct
    return comm_call(
        start_kernel,
        "start_gather",
        1,
        [
            shaped((peers,) + normed.shape, normed.dtype),
            shaped((peers,) + seq.shape, seq.dtype),
            shaped((sources,) + conv.shape, conv.dtype),
            shaped((planes,) + small.shape, small.dtype),
            shaped(cot.shape, cot.dtype),
        ],
        [dma(5)]
        + [dma(chips)] * 4
        + [dma(peers)] * 2
        + [dma(sources, chunks)] * 3
        + [dma(planes)] * 4,
        [normed, seq, conv, small, cot],
        size_of(normed) * peers,
    )


def all_sum_kernel(p_ref, out_ref, arrived, summed, own_sem, send, recv, wide_send, wide_recv):
    me = Place()
    greet(me, exp=False)
    first = []
    for k in range(1, me.peers):
        to = me.hid_at(k)
        copy = remote(p_ref.at[to], arrived.at[k], send.at[k], recv.at[k], me.e, to)
        copy.start()
        first.append(copy)
    total = p_ref[me.h].astype(jnp.float32)
    for k in range(1, me.peers):
        first[k - 1].wait_recv()
        total = total + arrived[k].astype(jnp.float32)
    summed[...] = total.astype(summed.dtype)
    own = pltpu.make_async_copy(summed, out_ref.at[me.h], own_sem)
    own.start()
    second = []
    for k in range(1, me.peers):
        copy = remote(
            summed, out_ref.at[me.h], wide_send.at[k], wide_recv.at[k], me.e, me.hid_at(k)
        )
        copy.start()
        second.append(copy)
    for k in range(1, me.peers):
        remote(
            summed, out_ref.at[me.hid_back(k)], wide_send.at[k], wide_recv.at[k], me.e, me.h
        ).wait_recv()
    for copy in first + second:
        copy.wait_send()
    own.wait()


def all_sum_hid(partial, out_type, name, collective_id):
    peers = lax.axis_size("hid")
    blocks = partial.reshape((peers, partial.shape[0] // peers) + partial.shape[1:])
    return comm_call(
        all_sum_kernel,
        name,
        collective_id,
        [jax.ShapeDtypeStruct(blocks.shape, out_type)],
        [
            pltpu.VMEM(blocks.shape, partial.dtype),
            pltpu.VMEM(blocks.shape[1:], out_type),
            pltpu.SemaphoreType.DMA,
        ]
        + [dma(peers)] * 4,
        [blocks],
        2 * size_of(blocks),
    )[0].reshape(partial.shape)


def scatter_pair(me, p_ref, mate, send, recv):
    copies = []
    for q in range(1, me.chips + 1):
        chip = me.chip_at(q)
        copy = remote(
            p_ref.at[2 * chip + 1 - me.core],
            mate.at[q % me.chips],
            send.at[q % me.chips],
            recv.at[q % me.chips],
            me.e,
            me.sibling,
        )
        copy.start()
        copies.append(copy)
    return copies


def scatter_chips(me, p_ref, mate, arrived, send, recv, pair_copies):
    copies = []
    for q in range(1, me.chips):
        chip = me.chip_at(q)
        pair_copies[q - 1].wait_recv()
        mate[q] = (
            mate[q].astype(jnp.float32) + p_ref[2 * chip + me.core].astype(jnp.float32)
        ).astype(mate.dtype)
        copy = remote(
            mate.at[q], arrived.at[q], send.at[q], recv.at[q], me.e, me.same_core(chip)
        )
        copy.start()
        copies.append(copy)
    return copies


def scatter_total(me, p_ref, mate, arrived, pair_copies, chip_copies):
    pair_copies[me.chips - 1].wait_recv()
    total = p_ref[me.h].astype(jnp.float32) + mate[0].astype(jnp.float32)
    for q in range(1, me.chips):
        chip_copies[q - 1].wait_recv()
        total = total + arrived[q].astype(jnp.float32)
    return total


def scatter_kernel(p_ref, out_ref, mate, arrived, pair_send, pair_recv, send, recv):
    me = Place()
    greet(me, exp=False)
    pair = scatter_pair(me, p_ref, mate, pair_send, pair_recv)
    far = scatter_chips(me, p_ref, mate, arrived, send, recv, pair)
    out_ref[...] = scatter_total(me, p_ref, mate, arrived, pair, far)
    for copy in pair + far:
        copy.wait_send()


def scatter_hid(partial, name, collective_id):
    peers = lax.axis_size("hid")
    chips = peers // 2
    blocks = partial.reshape((peers, partial.shape[0] // peers) + partial.shape[1:])
    landing = pltpu.VMEM((chips,) + blocks.shape[1:], partial.dtype)
    return comm_call(
        scatter_kernel,
        name,
        collective_id,
        [jax.ShapeDtypeStruct(blocks.shape[1:], jnp.float32)],
        [landing, landing] + [dma(chips)] * 4,
        [blocks],
        2 * size_of(blocks),
    )[0]


def dispatch_kernel(
    slots_ref, out_ref, own_sem, far_send, far_recv, chip_send, chip_recv, mate_send, mate_recv
):
    me = Place()
    greet(me)
    own = pltpu.make_async_copy(slots_ref.at[me.e], out_ref.at[me.e, me.core, me.chip], own_sem)
    own.start()
    sent = []
    for k in range(1, me.planes):
        to = me.plane_at(k)
        copy = remote(
            slots_ref.at[to],
            out_ref.at[me.e, me.core, me.chip],
            far_send.at[k],
            far_recv.at[k],
            to,
            me.h,
        )
        copy.start()
        sent.append(copy)

    for k in range(me.planes):
        source = me.plane_back(k)
        block = out_ref.at[source, me.core, me.chip]
        if k == 0:
            origin = slots_ref.at[me.e]
        else:
            origin = block
            remote(block, block, far_send.at[k], far_recv.at[k], me.e, me.h).wait_recv()
        for q in range(1, me.chips):
            copy = remote(
                origin,
                block,
                chip_send.at[k, q],
                chip_recv.at[k, q],
                me.e,
                me.same_core(me.chip_at(q)),
            )
            copy.start()
            sent.append(copy)
        copy = remote(origin, block, mate_send.at[k, 0], mate_recv.at[k, 0], me.e, me.sibling)
        copy.start()
        sent.append(copy)
    for k in range(me.planes):
        source = me.plane_back(k)
        for q in range(1, me.chips):
            block = out_ref.at[source, me.core, me.chip_back(q)]
            remote(block, block, chip_send.at[k, q], chip_recv.at[k, q], me.e, me.h).wait_recv()
            copy = remote(
                block, block, mate_send.at[k, q], mate_recv.at[k, q], me.e, me.sibling
            )
            copy.start()
            sent.append(copy)
    for k in range(me.planes):
        source = me.plane_back(k)
        for q in range(me.chips):
            block = out_ref.at[source, 1 - me.core, me.chip_back(q)]
            remote(block, block, mate_send.at[k, q], mate_recv.at[k, q], me.e, me.h).wait_recv()
    for copy in sent:
        copy.wait_send()
    own.wait()


def dispatch(slots, name, collective_id):
    planes, peers = lax.axis_size("exp"), lax.axis_size("hid")
    chips = peers // 2
    return comm_call(
        dispatch_kernel,
        name,
        collective_id,
        [jax.ShapeDtypeStruct((planes, 2, chips) + slots.shape[1:], slots.dtype)],
        [pltpu.SemaphoreType.DMA] + [dma(planes)] * 2 + [dma(planes, chips)] * 4,
        [slots],
        size_of(slots) * peers,
    )[0]


def give_back_kernel(
    a_ref,
    b_ref,
    a_out,
    b_out,
    a_mate,
    b_mate,
    a_in,
    b_in,
    a_sum,
    b_sum,
    pair_send,
    pair_recv,
    chip_send,
    chip_recv,
    far_send,
    far_recv,
):
    me = Place()
    planes, chips = me.planes, me.chips
    greet(me)
    parts = ((a_ref, a_out, a_mate, a_in, a_sum), (b_ref, b_out, b_mate, b_in, b_sum))
    sent, pair, cross = [], {}, {}
    for i in range(planes):
        to = me.plane_at(i + 1)
        for w, (p_ref, _, mate, _, _) in enumerate(parts):
            copy = remote(
                p_ref.at[to, 1 - me.core],
                mate.at[i],
                pair_send.at[w, i],
                pair_recv.at[w, i],
                me.e,
                me.sibling,
            )
            copy.start()
            pair[w, i] = copy
    for i in range(planes):
        to = me.plane_at(i + 1)
        for w, (p_ref, _, mate, arrived, _) in enumerate(parts):
            pair[w, i].wait_recv()

            def add(chip, carry, p_ref=p_ref, mate=mate, to=to, i=i):
                mate[i, chip] = (
                    mate[i, chip].astype(jnp.float32)
                    + p_ref[to, me.core, chip].astype(jnp.float32)
                ).astype(mate.dtype)
                return carry

            lax.fori_loop(0, chips, add, 0)
            for q in range(1, chips):
                chip = me.chip_at(q)
                copy = remote(
                    mate.at[i, chip],
                    arrived.at[i, q],
                    chip_send.at[w, i, q],
                    chip_recv.at[w, i, q],
                    me.e,
                    me.same_core(chip),
                )
                copy.start()
                cross[w, i, q] = copy
    for i in range(planes):
        to = me.plane_at(i + 1)
        for w, (_, out_ref, mate, arrived, summed) in enumerate(parts):
            total = mate[i, me.chip].astype(jnp.float32)
            for q in range(1, chips):
                cross[w, i, q].wait_recv()
                total = total + arrived[i, q].astype(jnp.float32)
            if i == planes - 1:
                out_ref[me.e] = total.astype(out_ref.dtype)
            else:
                summed[i] = total.astype(summed.dtype)
                copy = remote(
                    summed.at[i],
                    out_ref.at[me.e],
                    far_send.at[w, i],
                    far_recv.at[w, i],
                    to,
                    me.h,
                )
                copy.start()
                sent.append(copy)
    for i in range(planes - 1):
        for w, (_, out_ref, _, _, summed) in enumerate(parts):
            remote(
                summed.at[i],
                out_ref.at[me.plane_back(i + 1)],
                far_send.at[w, i],
                far_recv.at[w, i],
                me.e,
                me.h,
            ).wait_recv()
    for copy in sent + list(pair.values()) + list(cross.values()):
        copy.wait_send()


def give_back(a_part, b_part, name, collective_id):
    planes, peers = lax.axis_size("exp"), lax.axis_size("hid")
    chips = peers // 2
    shape = a_part.shape
    capacity, model_width = shape[-2:]
    kind = a_part.dtype
    out = jax.ShapeDtypeStruct((planes, capacity, model_width), kind)
    landing = pltpu.VMEM((planes, chips, capacity, model_width), kind)
    summed = pltpu.VMEM((planes, capacity, model_width), kind)
    return comm_call(
        give_back_kernel,
        name,
        collective_id,
        [out, out],
        [landing] * 4
        + [summed] * 2
        + [dma(2, planes)] * 2
        + [dma(2, planes, chips)] * 2
        + [dma(2, planes)] * 2,
        [a_part, b_part],
        2 * size_of(a_part),
    )


def finish_kernel(
    p_ref,
    conv_ref,
    small_ref,
    gain_ref,
    rows_out,
    conv_out,
    small_out,
    gain_out,
    mate,
    arrived,
    from_right,
    from_left,
    to_left,
    to_right,
    small_in,
    gain_in,
    gain_mid,
    gain_far,
    pair_send,
    pair_recv,
    send,
    recv,
    line_send,
    right_recv,
    left_recv,
    small_send,
    small_recv,
    gain_send,
    gain_recv,
    wide_send,
    wide_recv,
):
    me = Place()
    planes, peers = me.planes, me.peers
    targets, chunks = conv_ref.shape[0], conv_ref.shape[1]
    flat = me.e * peers + me.h
    half = flat // 2
    user = half % peers
    my_slot = 2 * (half // peers) + flat % 2
    self_user = user == me.h

    barrier = pltpu.get_barrier_semaphore()
    for k in range(1, peers):
        signal(barrier, me.e, me.hid_at(k))
    for k in range(1, planes):
        signal(barrier, me.plane_at(k), me.h)
    for k in range(1, planes):
        signal(barrier, me.plane_at(k), user)

    @pl.when(user != me.h)
    def _():
        signal(barrier, me.e, user)

    pl.semaphore_wait(barrier, peers - 1 + planes - 1 + planes - self_user.astype(jnp.int32))

    pair = scatter_pair(me, p_ref, mate, pair_send, pair_recv)

    def leftward(block, chunk, src):
        return remote(
            src,
            from_right.at[block, chunk],
            line_send.at[block, chunk],
            right_recv.at[block, chunk],
            me.e - 1,
            me.h,
        )

    def rightward(block, chunk, src):
        return remote(
            src,
            from_left.at[block, chunk],
            line_send.at[block, chunk],
            left_recv.at[block, chunk],
            me.e + 1,
            me.h,
        )

    for block in range(targets):
        for chunk in range(chunks):

            @pl.when((me.e == planes - 1) & (block < me.e))
            def _():
                leftward(block, chunk, conv_ref.at[block, chunk]).start()

            @pl.when((me.e == 0) & (block > me.e))
            def _():
                rightward(block, chunk, conv_ref.at[block, chunk]).start()

    def owner(s):
        j = 2 * ((s // 2) * peers + me.h) + s % 2
        return j // peers, j % peers, j != flat

    def small_copy(s):
        plane, hid, _ = owner(s)
        return remote(
            small_ref.at[s], small_in.at[me.e], small_send.at[s], small_recv.at[me.e], plane, hid
        )

    for s in range(planes):
        _, _, other = owner(s)

        @pl.when(other)
        def _():
            small_copy(s).start()

    gains = []
    for k in range(1, peers):
        copy = remote(
            gain_ref, gain_in.at[k], gain_send.at[k], gain_recv.at[k], me.e, me.hid_at(k)
        )
        copy.start()
        gains.append(copy)

    far = scatter_chips(me, p_ref, mate, arrived, send, recv, pair)

    total = gain_ref[...]
    for k in range(1, peers):
        gains[k - 1].wait_recv()
        total = total + gain_in[k]
    gain_mid[...] = total
    wide = []
    for k in range(1, planes):
        copy = remote(
            gain_mid, gain_far.at[k], wide_send.at[k], wide_recv.at[k], me.plane_at(k), me.h
        )
        copy.start()
        wide.append(copy)

    for block in range(targets):
        for chunk in range(chunks):

            @pl.when((block < me.e) & (me.e < planes - 1))
            def _():
                leftward(block, chunk, to_left.at[block, chunk]).wait_recv()
                to_left[block, chunk] = (
                    from_right[block, chunk].astype(jnp.float32)
                    + conv_ref[block, chunk].astype(jnp.float32)
                ).astype(to_left.dtype)
                leftward(block, chunk, to_left.at[block, chunk]).start()

            @pl.when((block > me.e) & (me.e > 0))
            def _():
                rightward(block, chunk, to_right.at[block, chunk]).wait_recv()
                to_right[block, chunk] = (
                    from_left[block, chunk].astype(jnp.float32)
                    + conv_ref[block, chunk].astype(jnp.float32)
                ).astype(to_right.dtype)
                rightward(block, chunk, to_right.at[block, chunk]).start()

    rows_out[...] = scatter_total(me, p_ref, mate, arrived, pair, far)

    for block in range(targets):

        @pl.when(block == me.e)
        def _():
            conv_out[...] = conv_ref[block].astype(jnp.float32)
            for chunk in range(chunks):

                @pl.when(me.e < planes - 1)
                def _():
                    leftward(block, chunk, to_left.at[block, chunk]).wait_recv()
                    conv_out[chunk] = conv_out[chunk] + from_right[block, chunk].astype(
                        jnp.float32
                    )

                @pl.when(me.e > 0)
                def _():
                    rightward(block, chunk, to_right.at[block, chunk]).wait_recv()
                    conv_out[chunk] = conv_out[chunk] + from_left[block, chunk].astype(
                        jnp.float32
                    )

    @pl.when(me.e >= targets)
    def _():
        conv_out[...] = jnp.zeros_like(conv_out)

    @pl.when(self_user)
    def _():
        small_in[me.e] = small_ref[my_slot]

    for k in range(planes):
        plane = me.plane_at(k)

        def arrive(plane=plane):
            remote(
                small_ref.at[0], small_in.at[plane], small_send.at[0], small_recv.at[plane], me.e, me.h
            ).wait_recv()

        if k == 0:
            pl.when(user != me.h)(arrive)
        else:
            arrive()
    small_total = small_in[0]
    for plane in range(1, planes):
        small_total = small_total + small_in[plane]
    small_out[...] = small_total

    total = gain_mid[...]
    for k in range(1, planes):
        wide[k - 1].wait_recv()
        total = total + gain_far[k]
    gain_out[...] = total

    for copy in pair + far + gains + wide:
        copy.wait_send()
    for s in range(planes):
        _, _, other = owner(s)

        @pl.when(other)
        def _():
            small_copy(s).wait_send()

    for block in range(targets):
        for chunk in range(chunks):

            @pl.when(block < me.e)
            def _():
                leftward(block, chunk, to_left.at[block, chunk]).wait_send()

            @pl.when(block > me.e)
            def _():
                rightward(block, chunk, to_right.at[block, chunk]).wait_send()


def finish(rows_part, conv_part, small_part, gain_part):
    planes, peers = lax.axis_size("exp"), lax.axis_size("hid")
    chips = peers // 2
    blocks = rows_part.reshape((peers, rows_part.shape[0] // peers) + rows_part.shape[1:])
    targets, chunks = conv_part.shape[:2]
    shaped = jax.ShapeDtypeStruct
    landing = pltpu.VMEM((chips,) + blocks.shape[1:], rows_part.dtype)
    line = pltpu.VMEM(conv_part.shape, conv_part.dtype)
    gain = gain_part.shape
    return comm_call(
        finish_kernel,
        "finish",
        2,
        [
            shaped(blocks.shape[1:], jnp.float32),
            shaped(conv_part.shape[1:], jnp.float32),
            shaped(small_part.shape[1:], jnp.float32),
            shaped(gain, jnp.float32),
        ],
        [landing, landing, line, line, line, line]
        + [
            pltpu.VMEM(small_part.shape, small_part.dtype),
            pltpu.VMEM((peers,) + gain, jnp.float32),
            pltpu.VMEM(gain, jnp.float32),
            pltpu.VMEM((planes,) + gain, jnp.float32),
        ]
        + [dma(chips)] * 4
        + [dma(targets, chunks)] * 3
        + [dma(planes)] * 2
        + [dma(peers)] * 2
        + [dma(planes)] * 2,
        [blocks, conv_part, small_part, gain_part],
        2 * size_of(blocks),
    )


def routing(exp_count, hid_count, bit):
    blocks = range(bit, exp_count * hid_count, 2)
    return [(j, (j // 2 // hid_count) * hid_count + (j // 2) % hid_count) for j in blocks]


def per_device(
    tokens,
    route,
    seq_ids,
    cotangent,
    gain_one,
    gain_two,
    in_weight,
    conv_weight,
    conv_bias,
    x_weight,
    dt_weight,
    dt_bias,
    a_log,
    skip,
    out_weight,
    expert_in,
    expert_out,
):
    both = ("exp", "hid")
    exp_count = lax.axis_size("exp")
    hid_count = lax.axis_size("hid")
    row_count = tokens.shape[1]
    model_width = tokens.shape[2]
    own = x_weight.shape[0]
    width = own * exp_count
    length = row_count * hid_count
    rank = dt_weight.shape[0]
    states = a_log.shape[1]
    taps = conv_weight.shape[0]
    pairs = [routing(exp_count, hid_count, bit) for bit in range(2)]
    leading = lax.axis_index("exp") < exp_count // 2

    x_rows = tokens[0].astype(jnp.float32)
    gain_first = gain_one.astype(jnp.float32)
    gain_second = gain_two.astype(jnp.float32)
    back_low = cotangent[0]

    capacity = 5 * row_count // (4 * exp_count)
    slot_count = exp_count * capacity
    chosen = route[0, :, 0]
    picks = (chosen[:, None] == jnp.arange(exp_count, dtype=jnp.int32)[None]).astype(jnp.int32)
    ranks = jnp.cumsum(picks, axis=0) - 1
    slot_of = jnp.sum(picks * ranks, axis=1)
    place = (
        (chosen * capacity + slot_of)[:, None] == jnp.arange(slot_count, dtype=jnp.int32)[None]
    ).astype(jnp.bfloat16)

    def to_slots(rows):
        slots = mat_tn(place, rows).astype(jnp.bfloat16)
        return slots.reshape(exp_count, capacity, model_width)

    small = jnp.concatenate(
        [
            x_weight,
            dt_weight.T,
            a_log,
            conv_weight.T,
            conv_bias[:, None],
            dt_bias[:, None],
            skip[:, None],
        ],
        axis=1,
    )
    pad = -small.shape[1] % 128
    small = jnp.concatenate([small, jnp.zeros((own, pad), jnp.bfloat16)], axis=1)
    in_rows = in_weight.T
    normed_blocks, seq_blocks, conv_blocks, small_blocks, cot_slots = start_gather(
        rms_scale(x_rows, gain_first).astype(jnp.bfloat16),
        seq_ids,
        in_rows.reshape(2, own, model_width),
        small,
        to_slots(back_low),
    )
    passed = jnp.concatenate([lax.ppermute(out_weight, both, pairs[bit]) for bit in range(2)])
    late = lax.all_gather(jnp.where(leading, passed, in_rows), "exp", axis=0, tiled=True)
    w_out, w_gate = late[:width], late[width:]
    w_conv_in = conv_blocks.reshape(width, model_width)
    w_small = small_blocks.reshape(width, -1)
    at = 0
    w_x = w_small[:, at : at + rank + 2 * states]
    at += rank + 2 * states
    w_dt = w_small[:, at : at + rank]
    at += rank
    alog_rows = w_small[:, at : at + states]
    at += states
    tap_rows = w_small[:, at : at + taps].astype(jnp.float32).T
    at += taps
    conv_shift = w_small[:, at].astype(jnp.float32)
    step_bias = w_small[:, at + 1].astype(jnp.float32)
    skip_gain = w_small[:, at + 2].astype(jnp.float32)
    a_neg = -jnp.exp(alog_rows.astype(jnp.float32)).T
    a_two = a_neg * LOG2_E

    normed_low = normed_blocks.reshape(length, model_width)
    seq_row = seq_blocks.reshape(length)
    conv_in = mat_nt(normed_low, w_conv_in)
    gate_in = mat_nt(normed_low, w_gate)
    rim = taps - 1
    ext_rows = jnp.concatenate([jnp.zeros((rim, width), jnp.float32), conv_in], axis=0)
    ext_seq = jnp.concatenate([jnp.full((rim,), -1, jnp.int32), seq_row], axis=0)
    matches = [
        (ext_seq[k : k + length] == seq_row).astype(jnp.float32)[:, None] for k in range(taps)
    ]
    conv_out = conv_shift[None] + jnp.zeros_like(conv_in)
    for k in range(taps):
        conv_out = conv_out + tap_rows[k][None] * matches[k] * ext_rows[k : k + length]
    activated = jax.nn.silu(conv_out)
    act_low = activated.astype(jnp.bfloat16)
    x_double = all_sum_hid(mat_nn(act_low, w_x), jnp.float32, "sum_double", 3)
    dt_low = x_double[:, :rank].astype(jnp.bfloat16)
    bc = x_double[:, rank:].reshape(length // SUB, SUB, 2 * states).transpose(0, 2, 1)
    pre_step = mat_nt(dt_low, w_dt) + step_bias[None]
    step_size = jax.nn.softplus(pre_step)
    step_cut = jnp.where(matches[taps - 2] > 0.5, step_size, CUT_STEP)
    drive = step_size * activated
    scanned, starts = scan_forward(step_cut, drive, bc, a_two, row_count)
    state_out = scanned + skip_gain[None] * activated
    gate_silu = jax.nn.silu(gate_in)
    mixed_low = (state_out * gate_silu).astype(jnp.bfloat16)
    mixed_sum = scatter_hid(mat_nn(mixed_low, w_out).astype(jnp.bfloat16), "scatter_mixed", 4)
    hidden_one = x_rows + mixed_sum
    two_low = rms_scale(hidden_one, gain_second).astype(jnp.bfloat16)

    rows_piece = dispatch(to_slots(two_low), "dispatch", 5)
    ordered = rows_piece.shape
    rows_piece = rows_piece.reshape(-1, model_width)
    grads_piece = lax.all_gather(cot_slots, "hid", axis=0, tiled=False)
    grads_piece = grads_piece.reshape((hid_count // 2, 2) + cot_slots.shape)
    grads_piece = grads_piece.transpose(2, 1, 0, 3, 4).reshape(-1, model_width)
    first_slice = expert_in[0]
    second_slice = expert_out[0]
    pre_act = mat_nn(rows_piece, first_slice)
    hidden_piece = jax.nn.gelu(pre_act, approximate=False).astype(jnp.bfloat16)
    grad_piece = (mat_nt(grads_piece, second_slice) * gelu_slope(pre_act)).astype(jnp.bfloat16)
    grad_first = mat_tn(rows_piece, grad_piece)[None]
    grad_second = mat_tn(hidden_piece, grads_piece)[None]
    out_slots, grad_slots = give_back(
        mat_nn(hidden_piece, second_slice).astype(jnp.bfloat16).reshape(ordered),
        mat_nt(grad_piece, first_slice).astype(jnp.bfloat16).reshape(ordered),
        "give_back",
        6,
    )
    branch_two = mat_nn(place, out_slots.reshape(slot_count, model_width))
    grad_normed = mat_nn(place, grad_slots.reshape(slot_count, model_width))
    result = (hidden_one + branch_two).astype(jnp.bfloat16)[None]
    _, norm_two_pull = jax.vjp(rms_scale, hidden_one, gain_second)
    grad_h_norm, grad_gain_second = norm_two_pull(grad_normed)
    grad_hidden = back_low.astype(jnp.float32) + grad_h_norm

    grad_mix = gather_hid(grad_hidden.astype(jnp.bfloat16), "gather_grad", 7)
    grad_mix = grad_mix.reshape(length, model_width)
    grad_out_w = mat_tn(mixed_low, grad_mix)
    grad_mixed = mat_nt(grad_mix, w_out)
    grad_state_out = grad_mixed * gate_silu
    grad_gate = (grad_mixed * state_out * silu_slope(gate_in)).astype(jnp.bfloat16)
    late_sum = lax.psum_scatter(
        jnp.concatenate([grad_out_w, mat_tn(grad_gate, normed_low)]).astype(jnp.bfloat16),
        "exp",
        scatter_dimension=0,
        tiled=True,
    )
    backs = [[(target, source) for source, target in pairs[bit]] for bit in range(2)]
    out_sum = sum(
        lax.ppermute(late_sum[bit * own : (bit + 1) * own], both, backs[bit]).astype(jnp.float32)
        for bit in range(2)
    )
    grad_skip = jnp.sum(grad_state_out * activated, axis=0)
    grad_drive, grad_cut, gb_flat, gc_flat, grad_amat = scan_backward(
        step_cut, drive, grad_state_out, bc, a_two, starts, row_count
    )
    grad_b = gb_flat[:, 0, :].reshape(length, states)
    grad_c = gc_flat[:, 0, :].reshape(length, states)
    grad_step = grad_cut * LN_2 + grad_drive * activated
    grad_act = grad_state_out * skip_gain[None] + grad_drive * step_size
    grad_pre_step = (grad_step * jax.nn.sigmoid(pre_step)).astype(jnp.bfloat16)
    grad_dt_bias = jnp.sum(grad_pre_step.astype(jnp.float32), axis=0)
    grad_dt_w = mat_tn(grad_pre_step, dt_low)
    grad_double = all_sum_hid(
        jnp.concatenate([mat_nn(grad_pre_step, w_dt), grad_b, grad_c], axis=1),
        jnp.bfloat16,
        "sum_grad_double",
        8,
    )
    grad_x_w = mat_tn(act_low, grad_double)
    grad_act = grad_act + mat_nt(grad_double, w_x)
    grad_conv = grad_act * silu_slope(conv_out)
    ext_grad = jnp.concatenate([grad_conv, jnp.zeros((rim, width), jnp.float32)], axis=0)
    ext_after = jnp.concatenate([seq_row, jnp.full((rim,), -1, jnp.int32)], axis=0)
    grad_conv_in = jnp.zeros_like(grad_conv)
    tap_grads = []
    for k in range(taps):
        tap_grads.append(jnp.sum(grad_conv * matches[k] * ext_rows[k : k + length], axis=0))
        agree = (ext_after[rim - k : rim - k + length] == seq_row).astype(jnp.float32)[:, None]
        grad_conv_in = (
            grad_conv_in + tap_rows[k][None] * agree * ext_grad[rim - k : rim - k + length]
        )
    grad_conv_b = jnp.sum(grad_conv, axis=0)
    grad_conv_low = grad_conv_in.astype(jnp.bfloat16)
    grad_in_conv = mat_tn(grad_conv_low, normed_low).astype(jnp.bfloat16)
    grad_rows = mat_nn(grad_conv_low, w_conv_in) + mat_nn(grad_gate, w_gate)
    grad_gain_first = jnp.sum(grad_rows * normed_low.astype(jnp.float32), axis=0) / gain_first

    grad_small = jnp.concatenate(
        [
            grad_x_w,
            grad_dt_w,
            (grad_amat * a_neg).T,
            jnp.stack(tap_grads + [grad_conv_b, grad_dt_bias, grad_skip], axis=1),
            jnp.zeros((width, pad), jnp.float32),
        ],
        axis=1,
    )
    grad_normed_one, conv_sum, small_own, gain_sums = finish(
        grad_rows.astype(jnp.bfloat16),
        grad_in_conv.reshape(exp_count // 2, 2, own, model_width),
        grad_small.reshape(exp_count, own, -1),
        jnp.stack([grad_gain_first, grad_gain_second]),
    )
    _, norm_one_pull = jax.vjp(lambda rows: rms_scale(rows, gain_first), x_rows)
    grad_tokens = (grad_hidden + norm_one_pull(grad_normed_one)[0])[None]
    in_sum = jnp.where(
        leading, conv_sum.reshape(2 * own, model_width), late_sum.astype(jnp.float32)
    )
    at = rank + 2 * states
    at_alog = at + rank
    at_taps = at_alog + states
    at_bias = at_taps + taps
    return (
        result,
        grad_tokens,
        gain_sums[0],
        gain_sums[1],
        in_sum.T,
        small_own[:, at_taps:at_bias].T,
        small_own[:, at_bias],
        small_own[:, :at],
        small_own[:, at:at_alog].T,
        small_own[:, at_bias + 1],
        small_own[:, at_alog:at_taps],
        small_own[:, at_bias + 2],
        out_sum,
        grad_first,
        grad_second,
    )


def solution(mesh):
    flat = ("exp", "hid")
    return jax.shard_map(
        per_device,
        mesh=mesh,
        in_specs=(
            P("exp", "hid", None),
            P("exp", "hid", None),
            P("exp", "hid"),
            P("exp", "hid", None),
            P(),
            P(),
            P(None, flat),
            P(None, flat),
            P(flat),
            P(flat, None),
            P(None, flat),
            P(flat),
            P(flat, None),
            P(flat),
            P(flat, None),
            P("exp", None, "hid"),
            P("exp", "hid", None),
        ),
        out_specs=(
            P("exp", "hid", None),
            P("exp", "hid", None),
            P(),
            P(),
            P(None, flat),
            P(None, flat),
            P(flat),
            P(flat, None),
            P(None, flat),
            P(flat),
            P(flat, None),
            P(flat),
            P(flat, None),
            P("exp", None, "hid"),
            P("exp", "hid", None),
        ),
        check_vma=False,
    )
```
